128 devices in a mesh: gx: 8 (over x, core), gy: 16 (over y, z).
Axes of the slice: x: 4, y: 4, z: 4, core: 2. Of those that a mesh axis runs over, the one named last changes fastest.
Arguments:
- electric: float32 [3, 128, 256, 256], P(None, 'gx', 'gy'), may hold values from -6 to 6
- magnetic: float32 [3, 128, 256, 256], P(None, 'gx', 'gy'), may hold values from -6 to 6
- aux_electric: float32 [6, 128, 256, 256], P(None, 'gx', 'gy'), may hold values from -3 to 3
- aux_magnetic: float32 [6, 128, 256, 256], P(None, 'gx', 'gy'), may hold values from -3 to 3
- grades: int32 [3, 128, 256, 256], P(None, 'gx', 'gy'), may hold values from 0 to 3
- permittivity: float32 [128, 256, 256], P('gx', 'gy'), may hold values from 1 to 8
- dipole_cell: int32 [3, 65536], P(None, ('gx', 'gy')), may hold values from 0 to 255, as said below
- dipole_port: int32 [65536], P(('gx', 'gy')), may hold values from 0 to 511
- live_count: int32 [128], P(('gx', 'gy')), may hold values from 1 to 512, as said below
- injection: bfloat16 [65536, 512], P(('gx', 'gy')), may hold values from -0.25 to 0.25
- waveform: bfloat16 [512, 16], replicated, may hold values from -6 to 6
Outputs:
- electric_out: float32 [3, 128, 256, 256], P(None, 'gx', 'gy')
- magnetic_out: float32 [3, 128, 256, 256], P(None, 'gx', 'gy')
- port_power: float32 [16, 512], replicated
The draws below stay inside these ranges and needn't reach their ends.
Inputs may be any that keep to these rules, and one draw needn't show every extreme that they name: `dipole_cell`: slot s lies in the block of cells held by the device that holds slot s. The live slots of a device are its first live_count ones; some device has all 512 live.
All inputs are finite; a program needn't handle non-finite values.
Results may differ from the reference program's by a relative error of at most 0.0003.
Values sent between devices are 32-bit elements; how exact they have to be, the bound alone decides.
A program may use at most 128 MiB of HBM per device.

```python
import math
import jax
import jax.numpy as jnp
from jax import lax

CX = 16
CY = 16
NZ = 256
DIP_DEV = 512
STEPS = 16
PORTS = 512
NX = 128
NY = 256
DIPOLES = 65536


def draw_dipole_cell(key, part):
    across = NY // CY
    slots = jnp.arange(DIPOLES, dtype=jnp.int32)
    owner = slots // DIP_DEV
    row_block = owner // across
    col_block = owner % across
    key_x, key_y, key_z = jax.random.split(jax.random.fold_in(key, 11), 3)
    coord_x = row_block * CX + jax.random.randint(key_x, (DIPOLES,), 0, CX)
    coord_y = col_block * CY + jax.random.randint(key_y, (DIPOLES,), 0, CY)
    coord_z = jax.random.randint(key_z, (DIPOLES,), 0, NZ)
    return jnp.stack([coord_x, coord_y, coord_z]).astype(jnp.int32)


def draw_dipole_port(key, part):
    devices = DIPOLES // DIP_DEV
    share = PORTS // devices
    slots = jnp.arange(DIPOLES, dtype=jnp.int32)
    owner = slots // DIP_DEV
    key_near, key_far, key_pick = jax.random.split(jax.random.fold_in(key, 23), 3)
    near = owner * share + jax.random.randint(key_near, (DIPOLES,), 0, share)
    far = jax.random.randint(key_far, (DIPOLES,), 0, PORTS)
    pick = jax.random.randint(key_pick, (DIPOLES,), 0, 4)
    return jnp.where(pick == 0, far, near).astype(jnp.int32)


def draw_live_count(key, part):
    devices = DIPOLES // DIP_DEV
    key_one, key_two, key_full = jax.random.split(jax.random.fold_in(key, 37), 3)
    first = jax.random.randint(key_one, (devices,), 1, DIP_DEV + 1)
    second = jax.random.randint(key_two, (devices,), 1, DIP_DEV + 1)
    counts = jnp.minimum(first, second)
    full = jax.random.randint(key_full, (), 0, devices)
    return jnp.where(jnp.arange(devices) == full, DIP_DEV, counts).astype(jnp.int32)


def place_ends(values, own_key, least, top_value):
    spot = [jax.random.randint(jax.random.fold_in(own_key, axis), (), 0, length) for axis, length in enumerate(values.shape)]
    main_axis = values.shape.index(max(values.shape))
    next_to = spot[:main_axis] + [(spot[main_axis] + 1) % values.shape[main_axis]] + spot[main_axis + 1:]
    return values.at[tuple(spot)].set(least).at[tuple(next_to)].set(top_value)


def block_levels(rng, extent, cuts, least, top_value):
    loudness = 1.0
    for dim, blocks in cuts:
        steps = jax.random.uniform(jax.random.fold_in(jax.random.fold_in(rng, 6), dim), (blocks,), jnp.float32, least / len(cuts), top_value / len(cuts))
        loudness = loudness * jnp.repeat(jnp.exp(steps), extent[dim] // blocks).reshape((-1,) + (1,) * (len(extent) - 1 - dim))
    return loudness


def normal_values(rng, shape, width, limit, cuts=(), kind=jnp.bfloat16):
    values = jax.random.normal(rng, shape, jnp.float32) * width
    if len(cuts) > 0:
        values = block_levels(rng, shape, cuts, -0.22, 0.18) * values
    return jnp.clip(values, min=-limit, max=limit).astype(kind)


def setup_inputs(seed: int = 0) -> dict:
    keys = jax.random.split(jax.random.key(seed), 12)
    electric = normal_values(keys[0], (3, NX, NY, NZ), 1.0, 6.0, ((1, 8), (2, 16)), jnp.float32)
    magnetic = normal_values(keys[1], (3, NX, NY, NZ), 1.0, 6.0, ((1, 8), (2, 16)), jnp.float32)
    aux_electric = normal_values(keys[2], (6, NX, NY, NZ), 0.4, 3.0, ((1, 8), (2, 16)), jnp.float32)
    aux_magnetic = normal_values(keys[3], (6, NX, NY, NZ), 0.4, 3.0, ((1, 8), (2, 16)), jnp.float32)
    grades = place_ends(jax.random.randint(keys[4], (3, NX, NY, NZ), 0, 4), jax.random.fold_in(keys[4], 1), 0, 3).astype(jnp.int32)
    permittivity = jnp.clip(jnp.exp(math.log(8.0) - 2.0794415 * jax.random.uniform(keys[5], (NX, NY, NZ), jnp.float32) ** block_levels(keys[5], (NX, NY, NZ), ((0, 8), (1, 16)), -0.2, 0.2)), 1.0, 8.0)
    dipole_cell = draw_dipole_cell(jax.random.fold_in(keys[11], 71), 0)
    dipole_port = draw_dipole_port(jax.random.fold_in(keys[11], 71), 0)
    live_count = draw_live_count(jax.random.fold_in(keys[11], 71), 0)
    injection = normal_values(keys[9], (DIPOLES, PORTS), PORTS ** -0.5, 0.25, ((0, 128),))
    waveform = normal_values(keys[10], (PORTS, STEPS), 1.0, 6.0)
    return dict(electric=electric, magnetic=magnetic, aux_electric=aux_electric, aux_magnetic=aux_magnetic, grades=grades, permittivity=permittivity, dipole_cell=dipole_cell, dipole_port=dipole_port, live_count=live_count, injection=injection, waveform=waveform)


courant = 0.55
absorb_keep = (0.0, 0.92, 0.75, 0.45)
absorb_take = (0.0, -0.06, -0.18, -0.35)
derivative_pairs = ((2, 1), (1, 2), (0, 2), (2, 0), (1, 0), (0, 1))


def difference(values, axis, plane, forward):
    length = values.shape[axis]
    if plane is None:
        shape = list(values.shape)
        shape[axis] = 1
        plane = jnp.zeros(shape, values.dtype)
    if forward:
        after = jnp.concatenate([lax.slice_in_dim(values, 1, length, axis=axis), plane], axis)
        return after - values
    before = jnp.concatenate([plane, lax.slice_in_dim(values, 0, length - 1, axis=axis)], axis)
    return values - before


def grade_table(grades, table):
    result = jnp.zeros(grades.shape, jnp.float32)
    for level in range(1, 4):
        result = result + jnp.where(grades == level, table[level], 0.0)
    return result


def curl(field, auxiliary, keep, take, planes, forward):
    terms = []
    updated = []
    for number, (component, axis) in enumerate(derivative_pairs):
        plane = None
        if planes is not None and axis == 0:
            plane = planes[0][component - 1]
        if planes is not None and axis == 1:
            plane = planes[1][component // 2]
        slope = difference(field[component], axis, plane, forward)
        carried = keep[axis] * auxiliary[number] + take[axis] * slope
        terms.append(slope + carried)
        updated.append(carried)
    rotation = jnp.stack([terms[0] - terms[1], terms[2] - terms[3], terms[4] - terms[5]])
    return rotation, jnp.stack(updated)


def reference(electric, magnetic, aux_electric, aux_magnetic, grades, permittivity, dipole_cell, dipole_port, live_count, injection, waveform):
    keep = grade_table(grades, absorb_keep)
    take = grade_table(grades, absorb_take)
    slots = jnp.arange(DIPOLES, dtype=jnp.int32)
    live = ((slots % DIP_DEV) < live_count[slots // DIP_DEV]).astype(jnp.float32)
    current = jnp.dot(injection, waveform, preferred_element_type=jnp.float32) * live[:, None]
    flat_cell = (dipole_cell[0] * (NY * NZ) + dipole_cell[1] * NZ + dipole_cell[2]).astype(jnp.int32)
    factor = courant / permittivity
    powers = []
    for step in range(STEPS):
        rotation, aux_electric = curl(electric, aux_electric, keep, take, None, True)
        magnetic = magnetic - courant * rotation
        rotation, aux_magnetic = curl(magnetic, aux_magnetic, keep, take, None, False)
        electric = electric + factor * rotation
        current_now = current[:, step]
        flat_z = electric[2].reshape(-1).at[flat_cell].add(-courant * current_now)
        drive = current_now * flat_z[flat_cell]
        electric = jnp.concatenate([electric[0:2], flat_z.reshape(1, NX, NY, NZ)], 0)
        powers.append(jax.ops.segment_sum(drive, dipole_port, PORTS))
    return electric, magnetic, jnp.stack(powers)
```

```python
import functools

import jax
import jax.numpy as jnp
from jax import lax
from jax.experimental import pallas as pl
from jax.experimental.pallas import tpu as pltpu
from jax.sharding import PartitionSpec as P

MESH = pl.DeviceIdType.MESH
S = 0.55
KEEP = (0.0, 0.92, 0.75, 0.45)
TAKE = (0.0, -0.06, -0.18, -0.35)
BF = jnp.bfloat16


def table(grades, values):
    out = jnp.zeros(grades.shape, jnp.float32)
    for level in range(1, 4):
        out = jnp.where(grades == level, values[level], out)
    return out


def halves(value):
    high = value.astype(BF)
    low = (value - high.astype(jnp.float32)).astype(BF)
    return high, low


def dot_nt(a, b):
    return lax.dot_general(a, b, (((1,), (1,)), ((), ())), preferred_element_type=jnp.float32)


def dot_nn(a, b):
    return jnp.dot(a, b, preferred_element_type=jnp.float32)


def kernel(
    shape, steps,
    live_ref, e_hbm, h_hbm, me_hbm, mh_hbm, g_hbm, p_hbm, cell_ref, port_ref, inj_ref, wave_ref,
    eo_hbm, ho_hbm, pw_ref,
    E, H, ME, MH, G, KP, TK, FC, PR, cellT, depthT, curT, rec, J,
    ey_send, hy_send, ey_recv, hy_recv,
    load_sem, store_sem, send_sem, recv_sem,
):
    nx, ny, nz = shape
    gx, gy = lax.axis_index("gx"), lax.axis_index("gy")
    last_x, last_y = lax.axis_size("gx") - 1, lax.axis_size("gy") - 1
    x_low, x_high = gx > 0, gx < last_x
    y_low, y_high = gy > 0, gy < last_y
    sides = (
        (x_low, (gx - 1, gy)),
        (x_high, (gx + 1, gy)),
        (y_low, (gx, gy - 1)),
        (y_high, (gx, gy + 1)),
    )
    loads = [
        pltpu.make_async_copy(e_hbm, E.at[:, 0:nx], load_sem.at[0]),
        pltpu.make_async_copy(h_hbm, H.at[:, 1 : nx + 1], load_sem.at[1]),
        pltpu.make_async_copy(me_hbm, ME, load_sem.at[2]),
        pltpu.make_async_copy(mh_hbm, MH, load_sem.at[3]),
        pltpu.make_async_copy(g_hbm, G, load_sem.at[4]),
        pltpu.make_async_copy(p_hbm, PR, load_sem.at[5]),
    ]
    for copy in loads:
        copy.start()
    zero_plane = jnp.zeros((ny, nz), jnp.float32)
    for c in range(3):
        E[c, nx] = zero_plane
        H[c, 0] = zero_plane
    ey_recv[...] = jnp.zeros_like(ey_recv)
    hy_recv[...] = jnp.zeros_like(hy_recv)

    barrier = pltpu.get_barrier_semaphore()
    for ok, target in sides:
        @pl.when(ok)
        def _():
            pl.semaphore_signal(barrier, inc=1, device_id=target, device_id_type=MESH)

    slots = cell_ref.shape[1]
    cell = (cell_ref[0:1, :] - gx * nx) * ny + (cell_ref[1:2, :] - gy * ny)
    cellT[...] = (
        lax.broadcasted_iota(jnp.int32, (nx * ny, slots), 0) == cell
    ).astype(jnp.float32)
    depthT[...] = (
        lax.broadcasted_iota(jnp.int32, (nz, slots), 0) == cell_ref[2:3, :]
    ).astype(jnp.float32).astype(BF)
    live = lax.broadcasted_iota(jnp.int32, (1, slots), 1) < live_ref[0]
    curT[...] = jnp.where(live, dot_nt(wave_ref[...], inj_ref[...]), 0.0)

    for copy in loads:
        copy.wait()

    @pl.loop(0, nx)
    def _(x):
        for d in range(3):
            grades = G[d, x]
            KP[d, x] = table(grades, KEEP)
            TK[d, x] = table(grades, TAKE)
        FC[x] = S / PR[x]

    pl.semaphore_wait(barrier, sum(ok.astype(jnp.int32) for ok, _ in sides))

    row = lax.broadcasted_iota(jnp.int32, (ny, nz), 0)
    lane = lax.broadcasted_iota(jnp.int32, (ny, nz), 1)

    def next_y(v):
        return jnp.where(row == ny - 1, 0.0, pltpu.roll(v, ny - 1, 0))

    def prev_y(v):
        return jnp.where(row == 0, 0.0, pltpu.roll(v, 1, 0))

    def next_z(v):
        return jnp.where(lane == nz - 1, 0.0, pltpu.roll(v, nz - 1, 1))

    def prev_z(v):
        return jnp.where(lane == 0, 0.0, pltpu.roll(v, 1, 1))

    def terms(slopes, memory, x):
        out = []
        for k, (slope, d) in enumerate(zip(slopes, (1, 2, 2, 0, 0, 1))):
            carried = KP[d, x] * memory[k, x] + TK[d, x] * slope
            memory[k, x] = carried
            out.append(slope + carried)
        return out

    def h_plane(x):
        ex, ey, ez = E[0, x], E[1, x], E[2, x]
        t = terms(
            (
                next_y(ez) - ez,
                next_z(ey) - ey,
                next_z(ex) - ex,
                E[2, x + 1] - ez,
                E[1, x + 1] - ey,
                next_y(ex) - ex,
            ),
            ME,
            x,
        )
        for c in range(3):
            H[c, x + 1] = H[c, x + 1] - S * (t[2 * c] - t[2 * c + 1])

    def e_plane(x):
        hx, hy, hz = H[0, x + 1], H[1, x + 1], H[2, x + 1]
        t = terms(
            (
                hz - prev_y(hz),
                hy - prev_z(hy),
                hx - prev_z(hx),
                hz - H[2, x],
                hy - H[1, x],
                hx - prev_y(hx),
            ),
            MH,
            x,
        )
        factor = FC[x]
        E[0, x] = E[0, x] + factor * (t[0] - t[1])
        E[1, x] = E[1, x] + factor * (t[2] - t[3])
        source = J[pl.ds(pl.multiple_of(x * ny, ny), ny), :]
        E[2, x] = E[2, x] + factor * (t[4] - t[5]) - source

    def remote(number, source, target_ref, target):
        return pltpu.make_async_remote_copy(
            src_ref=source,
            dst_ref=target_ref,
            send_sem=send_sem.at[number],
            recv_sem=recv_sem.at[number],
            device_id=target,
            device_id_type=MESH,
        )

    ex_copy = remote(0, E.at[1:3, 0], E.at[1:3, nx], (gx - 1, gy))
    ey_copy = remote(1, ey_send, ey_recv, (gx, gy - 1))
    hx_copy = remote(2, H.at[1:3, nx], H.at[1:3, 0], (gx + 1, gy))
    hy_copy = remote(3, hy_send, hy_recv, (gx, gy + 1))

    def drive(t):
        high, low = halves(E[2, 0:nx].reshape(nx * ny, nz))
        picked = dot_nn(high, depthT[...]) + dot_nn(low, depthT[...])
        value = jnp.sum(picked * cellT[...], axis=0, keepdims=True)
        rec[pl.ds(t, 1), :] = value * curT[pl.ds(t, 1), :]

    def sources(t):
        high, low = halves(S * curT[pl.ds(t, 1), :])
        mask = cellT[...].astype(BF)
        J[...] = dot_nt(mask * high, depthT[...]) + dot_nt(mask * low, depthT[...])

    @pl.loop(0, steps)
    def _(t):
        @pl.loop(0, nx)
        def _(x):
            ey_send[0, pl.ds(x, 1), :] = E[0, x, 0:1, :]
            ey_send[1, pl.ds(x, 1), :] = E[2, x, 0:1, :]

        @pl.when(x_low)
        def _():
            ex_copy.start()

        @pl.when(y_low)
        def _():
            ey_copy.start()

        @pl.loop(0, nx - 1)
        def _(x):
            h_plane(x)

        @pl.when(t > 0)
        def _():
            drive(t - 1)

        @pl.when(x_high)
        def _():
            ex_copy.wait_recv()

        h_plane(nx - 1)

        @pl.when(y_high)
        def _():
            ey_copy.wait_recv()

        @pl.loop(0, nx)
        def _(x):
            last = slice(ny - 1, ny)
            keep_take = TK[1, x, last, :]
            gx_row, gz_row = ey_recv[0, pl.ds(x, 1), :], ey_recv[1, pl.ds(x, 1), :]
            moved_z, moved_x = keep_take * gz_row, keep_take * gx_row
            ME[0, x, last, :] = ME[0, x, last, :] + moved_z
            ME[5, x, last, :] = ME[5, x, last, :] + moved_x
            new_x = H[0, x + 1, last, :] - S * (gz_row + moved_z)
            new_z = H[2, x + 1, last, :] + S * (gx_row + moved_x)
            H[0, x + 1, last, :] = new_x
            H[2, x + 1, last, :] = new_z
            hy_send[0, pl.ds(x, 1), :] = new_x
            hy_send[1, pl.ds(x, 1), :] = new_z

        @pl.when(x_high)
        def _():
            hx_copy.start()

        @pl.when(y_high)
        def _():
            hy_copy.start()

        sources(t)

        @pl.when(x_low)
        def _():
            ex_copy.wait_send()

        @pl.when(y_low)
        def _():
            ey_copy.wait_send()

        @pl.loop(1, nx)
        def _(x):
            e_plane(x)

        @pl.when(x_low)
        def _():
            hx_copy.wait_recv()

        e_plane(0)

        @pl.when(y_low)
        def _():
            hy_copy.wait_recv()

        @pl.loop(0, nx)
        def _(x):
            first = slice(0, 1)
            take_row, factor = TK[1, x, first, :], FC[x, first, :]
            hx_row, hz_row = hy_recv[0, pl.ds(x, 1), :], hy_recv[1, pl.ds(x, 1), :]
            moved_z, moved_x = take_row * hz_row, take_row * hx_row
            MH[0, x, first, :] = MH[0, x, first, :] - moved_z
            MH[5, x, first, :] = MH[5, x, first, :] - moved_x
            E[0, x, first, :] = E[0, x, first, :] - factor * (hz_row + moved_z)
            E[2, x, first, :] = E[2, x, first, :] + factor * (hx_row + moved_x)

        @pl.when(x_high)
        def _():
            hx_copy.wait_send()

        @pl.when(y_high)
        def _():
            hy_copy.wait_send()

    stores = [
        pltpu.make_async_copy(E.at[:, 0:nx], eo_hbm, store_sem.at[0]),
        pltpu.make_async_copy(H.at[:, 1 : nx + 1], ho_hbm, store_sem.at[1]),
    ]
    for copy in stores:
        copy.start()
    drive(steps - 1)
    ports = pw_ref.shape[1]
    members = (
        lax.broadcasted_iota(jnp.int32, (ports, slots), 0) == port_ref[...]
    ).astype(jnp.float32).astype(BF)
    high, low = halves(rec[...])
    pw_ref[...] = dot_nt(high, members) + dot_nt(low, members)
    for copy in stores:
        copy.wait()


def local(
    electric, magnetic, aux_electric, aux_magnetic, grades, permittivity,
    dipole_cell, dipole_port, live_count, injection, waveform,
):
    shape = electric.shape[1:]
    nx, ny, nz = shape
    slots = dipole_cell.shape[1]
    ports, steps = waveform.shape
    f32 = jnp.float32
    anywhere = pl.BlockSpec(memory_space=pl.ANY)
    vmem = pl.BlockSpec(memory_space=pltpu.VMEM)
    electric, magnetic, partial = pl.pallas_call(
        functools.partial(kernel, shape, steps),
        out_shape=(
            jax.ShapeDtypeStruct(electric.shape, f32),
            jax.ShapeDtypeStruct(magnetic.shape, f32),
            jax.ShapeDtypeStruct((steps, ports), f32),
        ),
        in_specs=[pl.BlockSpec(memory_space=pltpu.SMEM)] + [anywhere] * 6 + [vmem] * 4,
        out_specs=(anywhere, anywhere, vmem),
        scratch_shapes=[
            pltpu.VMEM((3, nx + 1, ny, nz), f32),
            pltpu.VMEM((3, nx + 1, ny, nz), f32),
            pltpu.VMEM((6, nx, ny, nz), f32),
            pltpu.VMEM((6, nx, ny, nz), f32),
            pltpu.VMEM((3, nx, ny, nz), jnp.int32),
            pltpu.VMEM((3, nx, ny, nz), f32),
            pltpu.VMEM((3, nx, ny, nz), f32),
            pltpu.VMEM((nx, ny, nz), f32),
            pltpu.VMEM((nx, ny, nz), f32),
            pltpu.VMEM((nx * ny, slots), f32),
            pltpu.VMEM((nz, slots), BF),
            pltpu.VMEM((steps, slots), f32),
            pltpu.VMEM((steps, slots), f32),
            pltpu.VMEM((nx * ny, nz), f32),
            pltpu.VMEM((2, nx, nz), f32),
            pltpu.VMEM((2, nx, nz), f32),
            pltpu.VMEM((2, nx, nz), f32),
            pltpu.VMEM((2, nx, nz), f32),
            pltpu.SemaphoreType.DMA((6,)),
            pltpu.SemaphoreType.DMA((2,)),
            pltpu.SemaphoreType.DMA((4,)),
            pltpu.SemaphoreType.DMA((4,)),
        ],
        compiler_params=pltpu.CompilerParams(
            collective_id=0, has_side_effects=True, vmem_limit_bytes=48 * 1024 * 1024
        ),
    )(
        live_count, electric, magnetic, aux_electric, aux_magnetic, grades, permittivity,
        dipole_cell, dipole_port.reshape(1, slots), injection, waveform.T,
    )
    return electric, magnetic, lax.psum(partial, ("gx", "gy"))


def solution(mesh):
    block = P(None, "gx", "gy", None)
    each = ("gx", "gy")
    return jax.shard_map(
        local,
        mesh=mesh,
        in_specs=(
            block, block, block, block, block, P("gx", "gy", None),
            P(None, each), P(each), P(each), P(each, None), P(),
        ),
        out_specs=(block, block, P()),
        check_vma=False,
    )
```

```python
import functools

import jax
import jax.numpy as jnp
from jax import lax
from jax.experimental import pallas as pl
from jax.experimental.pallas import tpu as pltpu
from jax.sharding import PartitionSpec as P

MESH = pl.DeviceIdType.MESH
S = 0.55
KEEP = (0.0, 0.92, 0.75, 0.45)
TAKE = (0.0, -0.06, -0.18, -0.35)
BF = jnp.bfloat16


def table(grades, values):
    out = jnp.zeros(grades.shape, jnp.float32)
    for level in range(1, 4):
        out = jnp.where(grades == level, values[level], out)
    return out


def halves(value):
    high = value.astype(BF)
    low = (value - high.astype(jnp.float32)).astype(BF)
    return high, low


def dot_nt(a, b):
    return lax.dot_general(a, b, (((1,), (1,)), ((), ())), preferred_element_type=jnp.float32)


def dot_nn(a, b):
    return jnp.dot(a, b, preferred_element_type=jnp.float32)


def kernel(
    shape, steps,
    live_ref, e_hbm, h_hbm, me_hbm, mh_hbm, g_hbm, p_hbm, cell_hbm, port_hbm, inj_hbm, wave_hbm,
    eo_hbm, ho_hbm, pw_ref,
    E, H, ME, MH, G, KP, TK, FC, PR, cellT, depthT, curT, rec, J,
    ey_send, hy_send, ey_recv, hy_recv, cell_ref, port_ref, inj_ref, wave_ref,
    part, half, ring, whole,
    load_sem, store_sem, send_sem, recv_sem, pair_send, pair_recv, ring_send, ring_recv,
):
    nx, ny, nz = shape
    gx, gy = lax.axis_index("gx"), lax.axis_index("gy")
    last_x, last_y = lax.axis_size("gx") - 1, lax.axis_size("gy") - 1
    x_low, x_high = gx > 0, gx < last_x
    y_low, y_high = gy > 0, gy < last_y
    sides = (
        (x_low, (gx - 1, gy)),
        (x_high, (gx + 1, gy)),
        (y_low, (gx, gy - 1)),
        (y_high, (gx, gy + 1)),
    )
    core, chip_x, chip_y, chip_z = gx % 2, gx // 2, gy // 4, gy % 4
    partner = (chip_x * 2 + 1 - core, gy)
    places = (chip_x, chip_y, chip_z)

    def fellow(axis, shift):
        if axis == 0:
            return ((chip_x + shift) % 4 * 2 + core, gy)
        if axis == 1:
            return (gx, (chip_y + shift) % 4 * 4 + chip_z)
        return (gx, chip_y * 4 + (chip_z + shift) % 4)

    small = [
        pltpu.make_async_copy(cell_hbm, cell_ref, load_sem.at[6]),
        pltpu.make_async_copy(port_hbm, port_ref, load_sem.at[7]),
        pltpu.make_async_copy(inj_hbm, inj_ref, load_sem.at[8]),
        pltpu.make_async_copy(wave_hbm, wave_ref, load_sem.at[9]),
    ]
    for copy in small:
        copy.start()
    loads = [
        pltpu.make_async_copy(e_hbm, E.at[:, 0:nx], load_sem.at[0]),
        pltpu.make_async_copy(h_hbm, H.at[:, 1 : nx + 1], load_sem.at[1]),
        pltpu.make_async_copy(me_hbm, ME, load_sem.at[2]),
        pltpu.make_async_copy(mh_hbm, MH, load_sem.at[3]),
        pltpu.make_async_copy(g_hbm, G, load_sem.at[4]),
        pltpu.make_async_copy(p_hbm, PR, load_sem.at[5]),
    ]
    for copy in loads:
        copy.start()
    zero_plane = jnp.zeros((ny, nz), jnp.float32)
    for c in range(3):
        E[c, nx] = zero_plane
        H[c, 0] = zero_plane
    ey_recv[...] = jnp.zeros_like(ey_recv)
    hy_recv[...] = jnp.zeros_like(hy_recv)

    barrier = pltpu.get_barrier_semaphore()
    for ok, target in sides:
        @pl.when(ok)
        def _():
            pl.semaphore_signal(barrier, inc=1, device_id=target, device_id_type=MESH)

    friends = [partner] + [fellow(axis, shift) for axis in range(3) for shift in range(1, 4)]
    for target in friends:
        pl.semaphore_signal(barrier, inc=1, device_id=target, device_id_type=MESH)
    for copy in small:
        copy.wait()
    slots = cell_ref.shape[1]
    cell = (cell_ref[0:1, :] - gx * nx) * ny + (cell_ref[1:2, :] - gy * ny)
    cellT[...] = (
        lax.broadcasted_iota(jnp.int32, (nx * ny, slots), 0) == cell
    ).astype(jnp.float32)
    depthT[...] = (
        lax.broadcasted_iota(jnp.int32, (nz, slots), 0) == cell_ref[2:3, :]
    ).astype(jnp.float32).astype(BF)
    live = lax.broadcasted_iota(jnp.int32, (1, slots), 1) < live_ref[0]
    curT[...] = jnp.where(live, dot_nt(wave_ref[...], inj_ref[...]), 0.0)

    for copy in loads:
        copy.wait()

    @pl.loop(0, nx)
    def _(x):
        for d in range(3):
            grades = G[d, x]
            KP[d, x] = table(grades, KEEP)
            TK[d, x] = table(grades, TAKE)
        FC[x] = S / PR[x]

    pl.semaphore_wait(barrier, sum(ok.astype(jnp.int32) for ok, _ in sides) + len(friends))

    row = lax.broadcasted_iota(jnp.int32, (ny, nz), 0)
    lane = lax.broadcasted_iota(jnp.int32, (ny, nz), 1)

    def next_y(v):
        return jnp.where(row == ny - 1, 0.0, pltpu.roll(v, ny - 1, 0))

    def prev_y(v):
        return jnp.where(row == 0, 0.0, pltpu.roll(v, 1, 0))

    def next_z(v):
        return jnp.where(lane == nz - 1, 0.0, pltpu.roll(v, nz - 1, 1))

    def prev_z(v):
        return jnp.where(lane == 0, 0.0, pltpu.roll(v, 1, 1))

    def terms(slopes, memory, x):
        out = []
        for k, (slope, d) in enumerate(zip(slopes, (1, 2, 2, 0, 0, 1))):
            carried = KP[d, x] * memory[k, x] + TK[d, x] * slope
            memory[k, x] = carried
            out.append(slope + carried)
        return out

    def h_plane(x):
        ex, ey, ez = E[0, x], E[1, x], E[2, x]
        t = terms(
            (
                next_y(ez) - ez,
                next_z(ey) - ey,
                next_z(ex) - ex,
                E[2, x + 1] - ez,
                E[1, x + 1] - ey,
                next_y(ex) - ex,
            ),
            ME,
            x,
        )
        for c in range(3):
            H[c, x + 1] = H[c, x + 1] - S * (t[2 * c] - t[2 * c + 1])

    def e_plane(x):
        hx, hy, hz = H[0, x + 1], H[1, x + 1], H[2, x + 1]
        t = terms(
            (
                hz - prev_y(hz),
                hy - prev_z(hy),
                hx - prev_z(hx),
                hz - H[2, x],
                hy - H[1, x],
                hx - prev_y(hx),
            ),
            MH,
            x,
        )
        factor = FC[x]
        E[0, x] = E[0, x] + factor * (t[0] - t[1])
        E[1, x] = E[1, x] + factor * (t[2] - t[3])
        source = J[pl.ds(pl.multiple_of(x * ny, ny), ny), :]
        E[2, x] = E[2, x] + factor * (t[4] - t[5]) - source

    def remote(number, source, target_ref, target):
        return pltpu.make_async_remote_copy(
            src_ref=source,
            dst_ref=target_ref,
            send_sem=send_sem.at[number],
            recv_sem=recv_sem.at[number],
            device_id=target,
            device_id_type=MESH,
        )

    ex_copy = remote(0, E.at[1:3, 0], E.at[1:3, nx], (gx - 1, gy))
    ey_copy = remote(1, ey_send, ey_recv, (gx, gy - 1))
    hx_copy = remote(2, H.at[1:3, nx], H.at[1:3, 0], (gx + 1, gy))
    hy_copy = remote(3, hy_send, hy_recv, (gx, gy + 1))

    def drive(t):
        high, low = halves(E[2, 0:nx].reshape(nx * ny, nz))
        picked = dot_nn(high, depthT[...]) + dot_nn(low, depthT[...])
        value = jnp.sum(picked * cellT[...], axis=0, keepdims=True)
        rec[pl.ds(t, 1), :] = value * curT[pl.ds(t, 1), :]

    def sources(t):
        high, low = halves(S * curT[pl.ds(t, 1), :])
        mask = cellT[...].astype(BF)
        J[...] = dot_nt(mask * high, depthT[...]) + dot_nt(mask * low, depthT[...])

    @pl.loop(0, steps)
    def _(t):
        @pl.loop(0, nx)
        def _(x):
            ey_send[0, pl.ds(x, 1), :] = E[0, x, 0:1, :]
            ey_send[1, pl.ds(x, 1), :] = E[2, x, 0:1, :]

        @pl.when(x_low)
        def _():
            ex_copy.start()

        @pl.when(y_low)
        def _():
            ey_copy.start()

        @pl.loop(0, nx - 1)
        def _(x):
            h_plane(x)

        @pl.when(t > 0)
        def _():
            drive(t - 1)

        @pl.when(x_high)
        def _():
            ex_copy.wait_recv()

        h_plane(nx - 1)

        @pl.when(y_high)
        def _():
            ey_copy.wait_recv()

        @pl.loop(0, nx)
        def _(x):
            last = slice(ny - 1, ny)
            keep_take = TK[1, x, last, :]
            gx_row, gz_row = ey_recv[0, pl.ds(x, 1), :], ey_recv[1, pl.ds(x, 1), :]
            moved_z, moved_x = keep_take * gz_row, keep_take * gx_row
            ME[0, x, last, :] = ME[0, x, last, :] + moved_z
            ME[5, x, last, :] = ME[5, x, last, :] + moved_x
            new_x = H[0, x + 1, last, :] - S * (gz_row + moved_z)
            new_z = H[2, x + 1, last, :] + S * (gx_row + moved_x)
            H[0, x + 1, last, :] = new_x
            H[2, x + 1, last, :] = new_z
            hy_send[0, pl.ds(x, 1), :] = new_x
            hy_send[1, pl.ds(x, 1), :] = new_z

        @pl.when(x_high)
        def _():
            hx_copy.start()

        @pl.when(y_high)
        def _():
            hy_copy.start()

        sources(t)

        @pl.when(x_low)
        def _():
            ex_copy.wait_send()

        @pl.when(y_low)
        def _():
            ey_copy.wait_send()

        @pl.loop(1, nx)
        def _(x):
            e_plane(x)

        @pl.when(x_low)
        def _():
            hx_copy.wait_recv()

        e_plane(0)

        @pl.when(y_low)
        def _():
            hy_copy.wait_recv()

        @pl.loop(0, nx)
        def _(x):
            first = slice(0, 1)
            take_row, factor = TK[1, x, first, :], FC[x, first, :]
            hx_row, hz_row = hy_recv[0, pl.ds(x, 1), :], hy_recv[1, pl.ds(x, 1), :]
            moved_z, moved_x = take_row * hz_row, take_row * hx_row
            MH[0, x, first, :] = MH[0, x, first, :] - moved_z
            MH[5, x, first, :] = MH[5, x, first, :] - moved_x
            E[0, x, first, :] = E[0, x, first, :] - factor * (hz_row + moved_z)
            E[2, x, first, :] = E[2, x, first, :] + factor * (hx_row + moved_x)

        @pl.when(x_high)
        def _():
            hx_copy.wait_send()

        @pl.when(y_high)
        def _():
            hy_copy.wait_send()

    stores = [
        pltpu.make_async_copy(E.at[:, 0:nx], eo_hbm, store_sem.at[0]),
        pltpu.make_async_copy(H.at[:, 1 : nx + 1], ho_hbm, store_sem.at[1]),
    ]
    for copy in stores:
        copy.start()
    drive(steps - 1)
    rows, ports = half.shape
    members = (
        lax.broadcasted_iota(jnp.int32, (ports, slots), 0) == port_ref[...]
    ).astype(jnp.float32).astype(BF)
    high, low = halves(rec[...])
    total = dot_nt(high, members) + dot_nt(low, members)
    part[0] = total[0:rows]
    part[1] = total[rows : 2 * rows]

    def swap(number, source, target_ref):
        return pltpu.make_async_remote_copy(
            src_ref=source,
            dst_ref=target_ref,
            send_sem=pair_send.at[number],
            recv_sem=pair_recv.at[number],
            device_id=partner,
            device_id_type=MESH,
        )

    def send(axis, shift):
        return pltpu.make_async_remote_copy(
            src_ref=ring.at[axis, places[axis]],
            dst_ref=ring.at[axis, places[axis]],
            send_sem=ring_send.at[axis, shift],
            recv_sem=ring_recv.at[axis, shift],
            device_id=fellow(axis, shift),
            device_id_type=MESH,
        )

    def arrival(axis, shift):
        slot = (places[axis] + 4 - shift) % 4
        return pltpu.make_async_remote_copy(
            src_ref=ring.at[axis, slot],
            dst_ref=ring.at[axis, slot],
            send_sem=ring_send.at[axis, shift],
            recv_sem=ring_recv.at[axis, shift],
            device_id=fellow(axis, shift),
            device_id_type=MESH,
        )

    trade = swap(0, part.at[1 - core], half)
    trade.start()
    trade.wait()
    value = part[core] + half[...]
    for axis in range(3):
        ring[axis, places[axis]] = value
        for shift in range(1, 4):
            send(axis, shift).start()
        for shift in range(1, 4):
            arrival(axis, shift).wait_recv()
        value = (ring[axis, 0] + ring[axis, 1]) + (ring[axis, 2] + ring[axis, 3])
    whole[core] = value
    trade = swap(1, whole.at[core], whole.at[core])
    trade.start()
    for axis in range(3):
        for shift in range(1, 4):
            send(axis, shift).wait_send()
    trade.wait()
    pw_ref[0:rows] = whole[0]
    pw_ref[rows : 2 * rows] = whole[1]
    for copy in stores:
        copy.wait()


def local(
    electric, magnetic, aux_electric, aux_magnetic, grades, permittivity,
    dipole_cell, dipole_port, live_count, injection, waveform,
):
    shape = electric.shape[1:]
    nx, ny, nz = shape
    slots = dipole_cell.shape[1]
    ports, steps = waveform.shape
    f32 = jnp.float32
    anywhere = pl.BlockSpec(memory_space=pl.ANY)
    vmem = pl.BlockSpec(memory_space=pltpu.VMEM)
    half = (steps // 2, ports)
    return pl.pallas_call(
        functools.partial(kernel, shape, steps),
        out_shape=(
            jax.ShapeDtypeStruct(electric.shape, f32),
            jax.ShapeDtypeStruct(magnetic.shape, f32),
            jax.ShapeDtypeStruct((steps, ports), f32),
        ),
        in_specs=[pl.BlockSpec(memory_space=pltpu.SMEM)] + [anywhere] * 10,
        out_specs=(anywhere, anywhere, vmem),
        scratch_shapes=[
            pltpu.VMEM((3, nx + 1, ny, nz), f32),
            pltpu.VMEM((3, nx + 1, ny, nz), f32),
            pltpu.VMEM((6, nx, ny, nz), f32),
            pltpu.VMEM((6, nx, ny, nz), f32),
            pltpu.VMEM((3, nx, ny, nz), jnp.int32),
            pltpu.VMEM((3, nx, ny, nz), f32),
            pltpu.VMEM((3, nx, ny, nz), f32),
            pltpu.VMEM((nx, ny, nz), f32),
            pltpu.VMEM((nx, ny, nz), f32),
            pltpu.VMEM((nx * ny, slots), f32),
            pltpu.VMEM((nz, slots), BF),
            pltpu.VMEM((steps, slots), f32),
            pltpu.VMEM((steps, slots), f32),
            pltpu.VMEM((nx * ny, nz), f32),
            pltpu.VMEM((2, nx, nz), f32),
            pltpu.VMEM((2, nx, nz), f32),
            pltpu.VMEM((2, nx, nz), f32),
            pltpu.VMEM((2, nx, nz), f32),
            pltpu.VMEM((3, slots), jnp.int32),
            pltpu.VMEM((1, slots), jnp.int32),
            pltpu.VMEM((slots, ports), BF),
            pltpu.VMEM((steps, ports), BF),
            pltpu.VMEM((2,) + half, f32),
            pltpu.VMEM(half, f32),
            pltpu.VMEM((3, 4) + half, f32),
            pltpu.VMEM((2,) + half, f32),
            pltpu.SemaphoreType.DMA((10,)),
            pltpu.SemaphoreType.DMA((2,)),
            pltpu.SemaphoreType.DMA((4,)),
            pltpu.SemaphoreType.DMA((4,)),
            pltpu.SemaphoreType.DMA((2,)),
            pltpu.SemaphoreType.DMA((2,)),
            pltpu.SemaphoreType.DMA((3, 4)),
            pltpu.SemaphoreType.DMA((3, 4)),
        ],
        compiler_params=pltpu.CompilerParams(
            collective_id=0, has_side_effects=True, vmem_limit_bytes=67_043_328
        ),
    )(
        live_count, electric, magnetic, aux_electric, aux_magnetic, grades, permittivity,
        dipole_cell, dipole_port.reshape(1, slots), injection, waveform.T,
    )


def solution(mesh):
    block = P(None, "gx", "gy", None)
    each = ("gx", "gy")
    return jax.shard_map(
        local,
        mesh=mesh,
        in_specs=(
            block, block, block, block, block, P("gx", "gy", None),
            P(None, each), P(each), P(each), P(each, None), P(),
        ),
        out_specs=(block, block, P()),
        check_vma=False,
    )
```

```python
import functools

import jax
import jax.numpy as jnp
from jax import lax
from jax.experimental import pallas as pl
from jax.experimental.pallas import tpu as pltpu
from jax.sharding import PartitionSpec as P

MESH = pl.DeviceIdType.MESH
S = 0.55
KEEP = (0.0, 0.92, 0.75, 0.45)
TAKE = (0.0, -0.06, -0.18, -0.35)
BF = jnp.bfloat16
Y, X, Z = 0, 1, 2
SPOT = (X, Y, Z)
DIMS = (1, 2, 2, 0, 0, 1)


def table(grades, values):
    out = jnp.zeros(grades.shape, jnp.float32)
    for level in range(1, 4):
        out = jnp.where(grades == level, values[level], out)
    return out


def halves(value):
    high = value.astype(BF)
    low = (value - high.astype(jnp.float32)).astype(BF)
    return high, low


def dot_nt(a, b):
    return lax.dot_general(a, b, (((1,), (1,)), ((), ())), preferred_element_type=jnp.float32)


def dot_nn(a, b):
    return jnp.dot(a, b, preferred_element_type=jnp.float32)


def kernel(
    shape, steps,
    live_ref, e_hbm, h_hbm, me_hbm, mh_hbm, g_hbm, p_hbm, cell_hbm, port_hbm, inj_hbm, wave_hbm,
    eo_hbm, ho_hbm, pw_ref,
    E, H, ME, MH, G, KP, TK, FC, PR, cellT, depthT, curT, rec, J,
    y_low_in, y_high_in, x_low_in, x_high_in, turn_in, cross_in,
    x_low_out, x_high_out, turn_out, cross_out, edge_out, edge, edge_keep, edge_take,
    cell_ref, port_ref, inj_ref, wave_ref,
    part, half, ring, whole,
    load_sem, big_sem, store_sem, send_sem, recv_sem, first_send, first_recv,
    pair_send, pair_recv, ring_send, ring_recv,
):
    nx, ny, nz = shape
    gx, gy = lax.axis_index("gx"), lax.axis_index("gy")
    last_x, last_y = lax.axis_size("gx") - 1, lax.axis_size("gy") - 1
    x_low, x_high = gx > 0, gx < last_x
    y_low, y_high = gy > 0, gy < last_y
    turn_to = jnp.logical_and(x_high, y_low)
    cross_to = jnp.logical_and(x_low, y_high)
    sides = (
        (x_low, (gx - 1, gy)),
        (x_high, (gx + 1, gy)),
        (y_low, (gx, gy - 1)),
        (y_high, (gx, gy + 1)),
        (turn_to, (gx + 1, gy - 1)),
        (cross_to, (gx - 1, gy + 1)),
    )
    core, chip_x, chip_y, chip_z = gx % 2, gx // 2, gy // 4, gy % 4
    partner = (chip_x * 2 + 1 - core, gy)
    places = (chip_x, chip_y, chip_z)

    def fellow(axis, shift):
        if axis == 0:
            return ((chip_x + shift) % 4 * 2 + core, gy)
        if axis == 1:
            return (gx, (chip_y + shift) % 4 * 4 + chip_z)
        return (gx, chip_y * 4 + (chip_z + shift) % 4)

    small = [
        pltpu.make_async_copy(cell_hbm, cell_ref, load_sem.at[0]),
        pltpu.make_async_copy(port_hbm, port_ref, load_sem.at[1]),
        pltpu.make_async_copy(inj_hbm, inj_ref, load_sem.at[2]),
        pltpu.make_async_copy(wave_hbm, wave_ref, load_sem.at[3]),
    ]
    loads = []
    inner = slice(1, ny + 1)
    for x in range(nx):
        pairs = [(e_hbm.at[c, x], E.at[SPOT[c], inner, x]) for c in range(3)]
        pairs += [(h_hbm.at[c, x], H.at[SPOT[c], inner, x]) for c in range(3)]
        pairs += [
            (me_hbm.at[:, x], ME.at[:, inner, x]),
            (g_hbm.at[:, x], G.at[:, inner, x]),
            (mh_hbm.at[:, x], MH.at[:, :, x]),
            (p_hbm.at[x], PR.at[:, x]),
        ]
        loads += [
            pltpu.make_async_copy(source, target, big_sem.at[number, x])
            for number, (source, target) in enumerate(pairs)
        ]
    for copy in loads + small:
        copy.start()

    H[:, 0] = jnp.zeros((3, nx, nz), jnp.float32)
    ME[:, 0] = jnp.zeros((6, nx, nz), jnp.float32)
    G[:, 0] = jnp.zeros((3, nx, nz), jnp.int32)
    for ref in (y_low_in, y_high_in, x_low_in, x_high_in, turn_in, cross_in, edge):
        ref[...] = jnp.zeros_like(ref)
    barrier = pltpu.get_barrier_semaphore()
    for ok, target in sides:
        @pl.when(ok)
        def _():
            pl.semaphore_signal(barrier, inc=1, device_id=target, device_id_type=MESH)

    friends = [partner] + [fellow(axis, shift) for axis in range(3) for shift in range(1, 4)]
    for target in friends:
        pl.semaphore_signal(barrier, inc=1, device_id=target, device_id_type=MESH)

    def remote(source, target_ref, sent, received, target):
        return pltpu.make_async_remote_copy(
            src_ref=source,
            dst_ref=target_ref,
            send_sem=sent,
            recv_sem=received,
            device_id=target,
            device_id_type=MESH,
        )

    def face_copies(slot):
        def one(number, source, target_ref, target):
            return remote(
                source, target_ref.at[slot], send_sem.at[number], recv_sem.at[number, slot], target
            )

        return (
            (y_high, y_low, one(0, E.at[:, ny], y_low_in, (gx, gy + 1))),
            (y_low, y_high, one(1, E.at[1:3, 1], y_high_in, (gx, gy - 1))),
            (turn_to, cross_to, one(2, turn_out, turn_in, (gx + 1, gy - 1))),
            (cross_to, turn_to, one(3, cross_out, cross_in, (gx - 1, gy + 1))),
            (x_high, x_low, one(4, x_high_out, x_low_in, (gx + 1, gy))),
            (x_low, x_high, one(5, x_low_out, x_high_in, (gx - 1, gy))),
        )

    def each(copies, action):
        for sends, receives, copy in copies:
            @pl.when(receives if action == "wait_recv" else sends)
            def _():
                getattr(copy, action)()

    def pack(a):
        at = pl.ds(a, 1)
        for number, c in enumerate((Y, Z)):
            x_low_out[number, at, :] = E[c, a + 1, 0:1, :]
        for c in range(3):
            x_high_out[c, at, :] = E[c, a + 1, nx - 1 : nx, :]

    def pack_corners():
        turn_out[...] = E[X, 1, nx - 1 : nx, :]
        cross_out[...] = E[Y, ny, 0:1, :]

    for copy in loads:
        copy.wait()

    @pl.loop(0, ny)
    def _(a):
        pack(a)
        at, end = pl.ds(a, 1), slice(nx - 1, nx)
        edge_out[0, at, :] = H[Y, a + 1, end, :]
        edge_out[1, at, :] = H[Z, a + 1, end, :]
        for k in range(4):
            edge_out[2 + k, at, :] = ME[2 + k, a + 1, end, :]
        for d in range(3):
            edge_out[6 + d, at, :] = G[d, a + 1, end, :].astype(jnp.float32)

    pack_corners()
    pl.semaphore_wait(barrier, sum(ok.astype(jnp.int32) for ok, _ in sides) + len(friends))
    up = (gx, gy + 1)
    firsts = [
        (x_high, x_low, edge_out, edge, (gx + 1, gy)),
        (y_high, y_low, G.at[:, ny], G.at[:, 0], up),
        (y_high, y_low, H.at[1:3, ny], H.at[1:3, 0], up),
        (y_high, y_low, ME.at[0:2, ny], ME.at[0:2, 0], up),
        (y_high, y_low, ME.at[4:6, ny], ME.at[4:6, 0], up),
    ]
    firsts = [
        (sends, receives, remote(source, target_ref, first_send.at[i], first_recv.at[i], target))
        for i, (sends, receives, source, target_ref, target) in enumerate(firsts)
    ]
    each(firsts, "start")
    each(face_copies(0), "start")

    for copy in small:
        copy.wait()
    slots = cell_ref.shape[1]
    cell = (cell_ref[1:2, :] - gy * ny) * nx + (cell_ref[0:1, :] - gx * nx)
    cellT[...] = (
        lax.broadcasted_iota(jnp.int32, (nx * ny, slots), 0) == cell
    ).astype(jnp.float32)
    depthT[...] = (
        lax.broadcasted_iota(jnp.int32, (nz, slots), 0) == cell_ref[2:3, :]
    ).astype(jnp.float32).astype(BF)
    live = lax.broadcasted_iota(jnp.int32, (1, slots), 1) < live_ref[0]
    curT[...] = jnp.where(live, dot_nt(wave_ref[...], inj_ref[...]), 0.0)

    @pl.loop(0, ny)
    def _(a):
        for d in range(3):
            grades = G[d, a + 1]
            KP[d, a + 1] = table(grades, KEEP)
            TK[d, a + 1] = table(grades, TAKE)
        FC[a] = S / PR[a]

    each(firsts, "wait_recv")
    each(firsts, "wait_send")
    for d in range(3):
        KP[d, 0] = table(G[d, 0], KEEP)
        TK[d, 0] = table(G[d, 0], TAKE)
        edge_keep[d] = table(edge[6 + d], KEEP)
        edge_take[d] = table(edge[6 + d], TAKE)

    row = lax.broadcasted_iota(jnp.int32, (nx, nz), 0)
    lane = lax.broadcasted_iota(jnp.int32, (nx, nz), 1)
    x_scale = jnp.where(x_low, S, 0.0)
    y_scale = jnp.where(y_low, S, 0.0)

    def next_row(v, fill):
        return jnp.where(row == nx - 1, fill, pltpu.roll(v, nx - 1, 0))

    def prev_row(v, fill):
        return jnp.where(row == 0, fill, pltpu.roll(v, 1, 0))

    def next_z(v):
        return jnp.where(lane == nz - 1, 0.0, pltpu.roll(v, nz - 1, 1))

    def prev_z(v):
        return jnp.where(lane == 0, 0.0, pltpu.roll(v, 1, 1))

    def term(k, slope, memory, a, shift):
        d = DIMS[k]
        carried = KP[d, a + 1] * memory[k, a + shift] + TK[d, a + 1] * slope
        memory[k, a + shift] = carried
        return slope + carried

    def h_plane(a, slot, above_x, above_z):
        ex, ey, ez = E[X, a + 1], E[Y, a + 1], E[Z, a + 1]
        at = pl.ds(a, 1)
        slopes = (
            above_z - ez,
            next_z(ey) - ey,
            next_z(ex) - ex,
            next_row(ez, x_high_in[slot, 1, at, :]) - ez,
            next_row(ey, x_high_in[slot, 0, at, :]) - ey,
            above_x - ex,
        )
        t = [term(k, slope, ME, a, 1) for k, slope in enumerate(slopes)]
        for c in range(3):
            spot = SPOT[c]
            H[spot, a + 1] = H[spot, a + 1] - S * (t[2 * c] - t[2 * c + 1])

    def h_below(slot):
        ey, ex, ez = (y_low_in[slot, c] for c in range(3))
        t0 = term(0, E[Z, 1] - ez, ME, -1, 1)
        t1 = term(1, next_z(ey) - ey, ME, -1, 1)
        t4 = term(4, next_row(ey, cross_in_row(slot)) - ey, ME, -1, 1)
        t5 = term(5, E[X, 1] - ex, ME, -1, 1)
        H[X, 0] = H[X, 0] - y_scale * (t0 - t1)
        H[Z, 0] = H[Z, 0] - y_scale * (t4 - t5)

    def cross_in_row(slot):
        return cross_in[slot]

    def h_edge(slot):
        ey, ex, ez = (x_low_in[slot, c] for c in range(3))
        slopes = (
            next_z(ex) - ex,
            x_low_out[1] - ez,
            x_low_out[0] - ey,
            next_row(ex, 0.0) - ex,
        )
        t = []
        for k, slope in enumerate(slopes):
            d = DIMS[2 + k]
            carried = edge_keep[d] * edge[2 + k] + edge_take[d] * slope
            edge[2 + k] = carried
            t.append(slope + carried)
        edge[0] = edge[0] - x_scale * (t[0] - t[1])
        edge[1] = edge[1] - x_scale * (t[2] - t[3])

    def h_edge_end(slot):
        end = slice(ny - 1, ny)
        corner = turn_in[slot]
        moved = edge_take[1, end, :] * corner
        edge[5, end, :] = edge[5, end, :] + moved
        edge[1, end, :] = edge[1, end, :] + x_scale * (corner + moved)

    def e_plane(a):
        hx, hy, hz = H[X, a + 1], H[Y, a + 1], H[Z, a + 1]
        at = pl.ds(a, 1)
        slopes = (
            hz - H[Z, a],
            hy - prev_z(hy),
            hx - prev_z(hx),
            hz - prev_row(hz, edge[1, at, :]),
            hy - prev_row(hy, edge[0, at, :]),
            hx - H[X, a],
        )
        t = [term(k, slope, MH, a, 0) for k, slope in enumerate(slopes)]
        factor = FC[a]
        E[X, a + 1] = E[X, a + 1] + factor * (t[0] - t[1])
        E[Y, a + 1] = E[Y, a + 1] + factor * (t[2] - t[3])
        source = J[pl.ds(a * nx, nx), :]
        E[Z, a + 1] = E[Z, a + 1] + factor * (t[4] - t[5]) - source

    def drive(t):
        high, low = halves(E[Z, 1 : ny + 1].reshape(nx * ny, nz))
        picked = dot_nn(high, depthT[...]) + dot_nn(low, depthT[...])
        value = jnp.sum(picked * cellT[...], axis=0, keepdims=True)
        rec[pl.ds(t, 1), :] = value * curT[pl.ds(t, 1), :]

    def sources(t):
        high, low = halves(S * curT[pl.ds(t, 1), :])
        mask = cellT[...].astype(BF)
        J[...] = dot_nt(mask * high, depthT[...]) + dot_nt(mask * low, depthT[...])

    @pl.loop(0, steps)
    def _(t):
        slot = t % 2
        copies = face_copies(slot)

        @pl.when(t > 0)
        def _():
            drive(t - 1)

        sources(t)
        each(copies[4:], "wait_recv")
        each(copies[4:], "wait_send")
        h_edge(slot)

        @pl.loop(0, ny - 1)
        def _(a):
            h_plane(a, slot, E[X, a + 2], E[Z, a + 2])

        @pl.loop(1, ny - 1)
        def _(a):
            e_plane(a)
            pack(a)

        each(copies[:4], "wait_recv")
        each(copies[:4], "wait_send")
        h_below(slot)
        h_plane(ny - 1, slot, y_high_in[slot, 0], y_high_in[slot, 1])
        h_edge_end(slot)
        e_plane(0)
        e_plane(ny - 1)
        pack_corners()
        pack(0)
        pack(ny - 1)

        @pl.when(t < steps - 1)
        def _():
            each(face_copies(1 - slot), "start")

    stores = [
        pltpu.make_async_copy(field.at[SPOT[c], inner, x], out.at[c, x], store_sem.at[i, c, x])
        for i, (field, out) in enumerate(((E, eo_hbm), (H, ho_hbm)))
        for c in range(3)
        for x in range(nx)
    ]
    for copy in stores:
        copy.start()
    drive(steps - 1)
    rows, ports = half.shape
    members = (
        lax.broadcasted_iota(jnp.int32, (ports, slots), 0) == port_ref[...]
    ).astype(jnp.float32).astype(BF)
    high, low = halves(rec[...])
    total = dot_nt(high, members) + dot_nt(low, members)
    part[0] = total[0:rows]
    part[1] = total[rows : 2 * rows]

    def swap(number, source, target_ref):
        return pltpu.make_async_remote_copy(
            src_ref=source,
            dst_ref=target_ref,
            send_sem=pair_send.at[number],
            recv_sem=pair_recv.at[number],
            device_id=partner,
            device_id_type=MESH,
        )

    def send(axis, shift):
        return pltpu.make_async_remote_copy(
            src_ref=ring.at[axis, places[axis]],
            dst_ref=ring.at[axis, places[axis]],
            send_sem=ring_send.at[axis, shift],
            recv_sem=ring_recv.at[axis, shift],
            device_id=fellow(axis, shift),
            device_id_type=MESH,
        )

    def arrival(axis, shift):
        slot = (places[axis] + 4 - shift) % 4
        return pltpu.make_async_remote_copy(
            src_ref=ring.at[axis, slot],
            dst_ref=ring.at[axis, slot],
            send_sem=ring_send.at[axis, shift],
            recv_sem=ring_recv.at[axis, shift],
            device_id=fellow(axis, shift),
            device_id_type=MESH,
        )

    trade = swap(0, part.at[1 - core], half)
    trade.start()
    trade.wait()
    value = part[core] + half[...]
    for axis in range(3):
        ring[axis, places[axis]] = value
        for shift in range(1, 4):
            send(axis, shift).start()
        for shift in range(1, 4):
            arrival(axis, shift).wait_recv()
        value = (ring[axis, 0] + ring[axis, 1]) + (ring[axis, 2] + ring[axis, 3])
    whole[core] = value
    trade = swap(1, whole.at[core], whole.at[core])
    trade.start()
    for axis in range(3):
        for shift in range(1, 4):
            send(axis, shift).wait_send()
    trade.wait()
    pw_ref[0:rows] = whole[0]
    pw_ref[rows : 2 * rows] = whole[1]
    for copy in stores:
        copy.wait()


def local(
    electric, magnetic, aux_electric, aux_magnetic, grades, permittivity,
    dipole_cell, dipole_port, live_count, injection, waveform,
):
    shape = electric.shape[1:]
    nx, ny, nz = shape
    slots = dipole_cell.shape[1]
    ports, steps = waveform.shape
    f32 = jnp.float32
    anywhere = pl.BlockSpec(memory_space=pl.ANY)
    vmem = pl.BlockSpec(memory_space=pltpu.VMEM)
    half = (steps // 2, ports)
    return pl.pallas_call(
        functools.partial(kernel, shape, steps),
        out_shape=(
            jax.ShapeDtypeStruct(electric.shape, f32),
            jax.ShapeDtypeStruct(magnetic.shape, f32),
            jax.ShapeDtypeStruct((steps, ports), f32),
        ),
        in_specs=[pl.BlockSpec(memory_space=pltpu.SMEM)] + [anywhere] * 10,
        out_specs=(anywhere, anywhere, vmem),
        scratch_shapes=[
            pltpu.VMEM((3, ny + 1, nx, nz), f32),
            pltpu.VMEM((3, ny + 1, nx, nz), f32),
            pltpu.VMEM((6, ny + 1, nx, nz), f32),
            pltpu.VMEM((6, ny, nx, nz), f32),
            pltpu.VMEM((3, ny + 1, nx, nz), jnp.int32),
            pltpu.VMEM((3, ny + 1, nx, nz), f32),
            pltpu.VMEM((3, ny + 1, nx, nz), f32),
            pltpu.VMEM((ny, nx, nz), f32),
            pltpu.VMEM((ny, nx, nz), f32),
            pltpu.VMEM((nx * ny, slots), f32),
            pltpu.VMEM((nz, slots), BF),
            pltpu.VMEM((steps, slots), f32),
            pltpu.VMEM((steps, slots), f32),
            pltpu.VMEM((nx * ny, nz), f32),
            pltpu.VMEM((2, 3, nx, nz), f32),
            pltpu.VMEM((2, 2, nx, nz), f32),
            pltpu.VMEM((2, 3, ny, nz), f32),
            pltpu.VMEM((2, 2, ny, nz), f32),
            pltpu.VMEM((2, 1, nz), f32),
            pltpu.VMEM((2, 1, nz), f32),
            pltpu.VMEM((2, ny, nz), f32),
            pltpu.VMEM((3, ny, nz), f32),
            pltpu.VMEM((1, nz), f32),
            pltpu.VMEM((1, nz), f32),
            pltpu.VMEM((9, ny, nz), f32),
            pltpu.VMEM((9, ny, nz), f32),
            pltpu.VMEM((3, ny, nz), f32),
            pltpu.VMEM((3, ny, nz), f32),
            pltpu.VMEM((3, slots), jnp.int32),
            pltpu.VMEM((1, slots), jnp.int32),
            pltpu.VMEM((slots, ports), BF),
            pltpu.VMEM((steps, ports), BF),
            pltpu.VMEM((2,) + half, f32),
            pltpu.VMEM(half, f32),
            pltpu.VMEM((3, 4) + half, f32),
            pltpu.VMEM((2,) + half, f32),
            pltpu.SemaphoreType.DMA((4,)),
            pltpu.SemaphoreType.DMA((10, nx)),
            pltpu.SemaphoreType.DMA((2, 3, nx)),
            pltpu.SemaphoreType.DMA((6,)),
            pltpu.SemaphoreType.DMA((6, 2)),
            pltpu.SemaphoreType.DMA((5,)),
            pltpu.SemaphoreType.DMA((5,)),
            pltpu.SemaphoreType.DMA((2,)),
            pltpu.SemaphoreType.DMA((2,)),
            pltpu.SemaphoreType.DMA((3, 4)),
            pltpu.SemaphoreType.DMA((3, 4)),
        ],
        compiler_params=pltpu.CompilerParams(
            collective_id=0, has_side_effects=True, vmem_limit_bytes=67_043_328
        ),
    )(
        live_count, electric, magnetic, aux_electric, aux_magnetic, grades, permittivity,
        dipole_cell, dipole_port.reshape(1, slots), injection, waveform.T,
    )


def solution(mesh):
    block = P(None, "gx", "gy", None)
    each = ("gx", "gy")
    return jax.shard_map(
        local,
        mesh=mesh,
        in_specs=(
            block, block, block, block, block, P("gx", "gy", None),
            P(None, each), P(each), P(each), P(each, None), P(),
        ),
        out_specs=(block, block, P()),
        check_vma=False,
    )
```

```python
import functools

import jax
import jax.numpy as jnp
from jax import lax
from jax.experimental import pallas as pl
from jax.experimental.pallas import tpu as pltpu
from jax.sharding import PartitionSpec as P

MESH = pl.DeviceIdType.MESH
S = 0.55
KEEP = (0.0, 0.92, 0.75, 0.45)
TAKE = (0.0, -0.06, -0.18, -0.35)
BF = jnp.bfloat16
Y, X, Z = 0, 1, 2
SPOT = (X, Y, Z)
DIMS = (1, 2, 2, 0, 0, 1)


def table(grades, values):
    out = jnp.zeros(grades.shape, jnp.float32)
    for level in range(1, 4):
        out = jnp.where(grades == level, values[level], out)
    return out


def halves(value):
    high = value.astype(BF)
    low = (value - high.astype(jnp.float32)).astype(BF)
    return high, low


def dot_nt(a, b):
    return lax.dot_general(a, b, (((1,), (1,)), ((), ())), preferred_element_type=jnp.float32)


def dot_nn(a, b):
    return jnp.dot(a, b, preferred_element_type=jnp.float32)


def kernel(
    shape, steps,
    live_ref, e_hbm, h_hbm, me_hbm, mh_hbm, g_hbm, p_hbm, cell_hbm, port_hbm, inj_hbm, wave_hbm,
    eo_hbm, ho_hbm, pw_ref,
    E, H, ME, MH, G, KP, TK, FC, PR, cellT, depthT, curT, rec, J,
    y_low_in, y_high_in, x_low_in, x_high_in, turn_in, cross_in,
    x_low_out, x_high_out, turn_out, cross_out, edge_out, edge, edge_keep, edge_take,
    cell_ref, port_ref, inj_ref, wave_ref,
    part, half, ring, whole,
    load_sem, big_sem, store_sem, send_sem, recv_sem, first_send, first_recv,
    pair_send, pair_recv, ring_send, ring_recv,
):
    nx, ny, nz = shape
    gx, gy = lax.axis_index("gx"), lax.axis_index("gy")
    last_x, last_y = lax.axis_size("gx") - 1, lax.axis_size("gy") - 1
    x_low, x_high = gx > 0, gx < last_x
    y_low, y_high = gy > 0, gy < last_y
    turn_to = jnp.logical_and(x_high, y_low)
    cross_to = jnp.logical_and(x_low, y_high)
    sides = (
        (x_low, (gx - 1, gy)),
        (x_high, (gx + 1, gy)),
        (y_low, (gx, gy - 1)),
        (y_high, (gx, gy + 1)),
        (turn_to, (gx + 1, gy - 1)),
        (cross_to, (gx - 1, gy + 1)),
    )
    core, chip_x, chip_y, chip_z = gx % 2, gx // 2, gy // 4, gy % 4
    partner = (chip_x * 2 + 1 - core, gy)
    places = (chip_x, chip_y, chip_z)

    def fellow(axis, shift):
        if axis == 0:
            return ((chip_x + shift) % 4 * 2 + core, gy)
        if axis == 1:
            return (gx, (chip_y + shift) % 4 * 4 + chip_z)
        return (gx, chip_y * 4 + (chip_z + shift) % 4)

    small = [
        pltpu.make_async_copy(cell_hbm, cell_ref, load_sem.at[0]),
        pltpu.make_async_copy(port_hbm, port_ref, load_sem.at[1]),
        pltpu.make_async_copy(inj_hbm, inj_ref, load_sem.at[2]),
        pltpu.make_async_copy(wave_hbm, wave_ref, load_sem.at[3]),
    ]
    inner = slice(1, ny + 1)

    def plane_loads(a):
        pairs = [(e_hbm.at[c, :, a], E.at[SPOT[c], a + 1]) for c in range(3)]
        pairs += [(h_hbm.at[c, :, a], H.at[SPOT[c], a + 1]) for c in range(3)]
        pairs += [
            (me_hbm.at[:, :, a], ME.at[:, a + 1]),
            (g_hbm.at[:, :, a], G.at[:, a + 1]),
            (mh_hbm.at[:, :, a], MH.at[:, a]),
            (p_hbm.at[:, a], PR.at[a]),
        ]
        return [
            pltpu.make_async_copy(source, target, big_sem.at[number, a])
            for number, (source, target) in enumerate(pairs)
        ]

    top = plane_loads(ny - 1)
    loads = [copy for a in range(ny - 1) for copy in plane_loads(a)]
    for copy in top + loads + small:
        copy.start()

    H[:, 0] = jnp.zeros((3, nx, nz), jnp.float32)
    ME[:, 0] = jnp.zeros((6, nx, nz), jnp.float32)
    G[:, 0] = jnp.zeros((3, nx, nz), jnp.int32)
    for ref in (y_low_in, y_high_in, x_low_in, x_high_in, turn_in, cross_in, edge):
        ref[...] = jnp.zeros_like(ref)
    barrier = pltpu.get_barrier_semaphore()
    for ok, target in sides:
        @pl.when(ok)
        def _():
            pl.semaphore_signal(barrier, inc=1, device_id=target, device_id_type=MESH)

    friends = [partner] + [fellow(axis, shift) for axis in range(3) for shift in range(1, 4)]
    for target in friends:
        pl.semaphore_signal(barrier, inc=1, device_id=target, device_id_type=MESH)

    def remote(source, target_ref, sent, received, target):
        return pltpu.make_async_remote_copy(
            src_ref=source,
            dst_ref=target_ref,
            send_sem=sent,
            recv_sem=received,
            device_id=target,
            device_id_type=MESH,
        )

    def face_copies(slot):
        def one(number, source, target_ref, target):
            return remote(
                source, target_ref.at[slot], send_sem.at[number], recv_sem.at[number, slot], target
            )

        return (
            (y_high, y_low, one(0, E.at[:, ny], y_low_in, (gx, gy + 1))),
            (y_low, y_high, one(1, E.at[1:3, 1], y_high_in, (gx, gy - 1))),
            (turn_to, cross_to, one(2, turn_out, turn_in, (gx + 1, gy - 1))),
            (cross_to, turn_to, one(3, cross_out, cross_in, (gx - 1, gy + 1))),
            (x_high, x_low, one(4, x_high_out, x_low_in, (gx + 1, gy))),
            (x_low, x_high, one(5, x_low_out, x_high_in, (gx - 1, gy))),
        )

    def each(copies, action):
        for sends, receives, copy in copies:
            @pl.when(receives if action == "wait_recv" else sends)
            def _():
                getattr(copy, action)()

    def pack(a):
        at = pl.ds(a, 1)
        for number, c in enumerate((Y, Z)):
            x_low_out[number, at, :] = E[c, a + 1, 0:1, :]
        for c in range(3):
            x_high_out[c, at, :] = E[c, a + 1, nx - 1 : nx, :]

    def pack_corners():
        turn_out[...] = E[X, 1, nx - 1 : nx, :]
        cross_out[...] = E[Y, ny, 0:1, :]

    up = (gx, gy + 1)
    firsts = [
        (x_high, x_low, edge_out, edge, (gx + 1, gy)),
        (y_high, y_low, G.at[:, ny], G.at[:, 0], up),
        (y_high, y_low, H.at[1:3, ny], H.at[1:3, 0], up),
        (y_high, y_low, ME.at[0:2, ny], ME.at[0:2, 0], up),
        (y_high, y_low, ME.at[4:6, ny], ME.at[4:6, 0], up),
    ]
    firsts = [
        (sends, receives, remote(source, target_ref, first_send.at[i], first_recv.at[i], target))
        for i, (sends, receives, source, target_ref, target) in enumerate(firsts)
    ]
    for copy in top:
        copy.wait()
    pl.semaphore_wait(barrier, sum(ok.astype(jnp.int32) for ok, _ in sides) + len(friends))
    each(face_copies(0)[:1], "start")
    each(firsts[1:], "start")
    for copy in loads:
        copy.wait()

    @pl.loop(0, ny)
    def _(a):
        pack(a)
        at, end = pl.ds(a, 1), slice(nx - 1, nx)
        edge_out[0, at, :] = H[Y, a + 1, end, :]
        edge_out[1, at, :] = H[Z, a + 1, end, :]
        for k in range(4):
            edge_out[2 + k, at, :] = ME[2 + k, a + 1, end, :]
        for d in range(3):
            edge_out[6 + d, at, :] = G[d, a + 1, end, :].astype(jnp.float32)

    pack_corners()
    each(face_copies(0)[1:], "start")
    each(firsts[:1], "start")

    for copy in small:
        copy.wait()
    slots = cell_ref.shape[1]
    cell = (cell_ref[1:2, :] - gy * ny) * nx + (cell_ref[0:1, :] - gx * nx)
    cellT[...] = (
        lax.broadcasted_iota(jnp.int32, (nx * ny, slots), 0) == cell
    ).astype(jnp.float32)
    depthT[...] = (
        lax.broadcasted_iota(jnp.int32, (nz, slots), 0) == cell_ref[2:3, :]
    ).astype(jnp.float32).astype(BF)
    live = lax.broadcasted_iota(jnp.int32, (1, slots), 1) < live_ref[0]
    curT[...] = jnp.where(live, dot_nt(wave_ref[...], inj_ref[...]), 0.0)

    @pl.loop(0, ny)
    def _(a):
        for d in range(3):
            grades = G[d, a + 1]
            KP[d, a + 1] = table(grades, KEEP)
            TK[d, a + 1] = table(grades, TAKE)
        FC[a] = S / PR[a]

    row = lax.broadcasted_iota(jnp.int32, (nx, nz), 0)
    lane = lax.broadcasted_iota(jnp.int32, (nx, nz), 1)
    x_scale = jnp.where(x_low, S, 0.0)
    y_scale = jnp.where(y_low, S, 0.0)

    def next_row(v, fill):
        return jnp.where(row == nx - 1, fill, pltpu.roll(v, nx - 1, 0))

    def prev_row(v, fill):
        return jnp.where(row == 0, fill, pltpu.roll(v, 1, 0))

    def next_z(v):
        return jnp.where(lane == nz - 1, 0.0, pltpu.roll(v, nz - 1, 1))

    def prev_z(v):
        return jnp.where(lane == 0, 0.0, pltpu.roll(v, 1, 1))

    def term(k, slope, memory, a, shift):
        d = DIMS[k]
        carried = KP[d, a + 1] * memory[k, a + shift] + TK[d, a + 1] * slope
        memory[k, a + shift] = carried
        return slope + carried

    def h_plane(a, slot, above_x, above_z):
        ex, ey, ez = E[X, a + 1], E[Y, a + 1], E[Z, a + 1]
        at = pl.ds(a, 1)
        slopes = (
            above_z - ez,
            next_z(ey) - ey,
            next_z(ex) - ex,
            next_row(ez, x_high_in[slot, 1, at, :]) - ez,
            next_row(ey, x_high_in[slot, 0, at, :]) - ey,
            above_x - ex,
        )
        t = [term(k, slope, ME, a, 1) for k, slope in enumerate(slopes)]
        for c in range(3):
            spot = SPOT[c]
            H[spot, a + 1] = H[spot, a + 1] - S * (t[2 * c] - t[2 * c + 1])

    def h_below(slot):
        ey, ex, ez = (y_low_in[slot, c] for c in range(3))
        t0 = term(0, E[Z, 1] - ez, ME, -1, 1)
        t1 = term(1, next_z(ey) - ey, ME, -1, 1)
        t4 = term(4, next_row(ey, cross_in_row(slot)) - ey, ME, -1, 1)
        t5 = term(5, E[X, 1] - ex, ME, -1, 1)
        H[X, 0] = H[X, 0] - y_scale * (t0 - t1)
        H[Z, 0] = H[Z, 0] - y_scale * (t4 - t5)

    def cross_in_row(slot):
        return cross_in[slot]

    def h_edge(slot):
        ey, ex, ez = (x_low_in[slot, c] for c in range(3))
        slopes = (
            next_z(ex) - ex,
            x_low_out[1] - ez,
            x_low_out[0] - ey,
            next_row(ex, 0.0) - ex,
        )
        t = []
        for k, slope in enumerate(slopes):
            d = DIMS[2 + k]
            carried = edge_keep[d] * edge[2 + k] + edge_take[d] * slope
            edge[2 + k] = carried
            t.append(slope + carried)
        edge[0] = edge[0] - x_scale * (t[0] - t[1])
        edge[1] = edge[1] - x_scale * (t[2] - t[3])

    def h_edge_end(slot):
        end = slice(ny - 1, ny)
        corner = turn_in[slot]
        moved = edge_take[1, end, :] * corner
        edge[5, end, :] = edge[5, end, :] + moved
        edge[1, end, :] = edge[1, end, :] + x_scale * (corner + moved)

    def e_plane(a):
        hx, hy, hz = H[X, a + 1], H[Y, a + 1], H[Z, a + 1]
        at = pl.ds(a, 1)
        slopes = (
            hz - H[Z, a],
            hy - prev_z(hy),
            hx - prev_z(hx),
            hz - prev_row(hz, edge[1, at, :]),
            hy - prev_row(hy, edge[0, at, :]),
            hx - H[X, a],
        )
        t = [term(k, slope, MH, a, 0) for k, slope in enumerate(slopes)]
        factor = FC[a]
        E[X, a + 1] = E[X, a + 1] + factor * (t[0] - t[1])
        E[Y, a + 1] = E[Y, a + 1] + factor * (t[2] - t[3])
        source = J[pl.ds(a * nx, nx), :]
        E[Z, a + 1] = E[Z, a + 1] + factor * (t[4] - t[5]) - source

    def drive(t):
        high, low = halves(E[Z, 1 : ny + 1].reshape(nx * ny, nz))
        picked = dot_nn(high, depthT[...]) + dot_nn(low, depthT[...])
        value = jnp.sum(picked * cellT[...], axis=0, keepdims=True)
        rec[pl.ds(t, 1), :] = value * curT[pl.ds(t, 1), :]

    def sources(t):
        high, low = halves(S * curT[pl.ds(t, 1), :])
        mask = cellT[...].astype(BF)
        J[...] = dot_nt(mask * high, depthT[...]) + dot_nt(mask * low, depthT[...])

    @pl.loop(0, steps)
    def _(t):
        slot = t % 2
        copies = face_copies(slot)

        @pl.when(t > 0)
        def _():
            drive(t - 1)

        sources(t)
        each(copies[4:], "wait_recv")
        each(copies[4:], "wait_send")

        @pl.when(t == 0)
        def _():
            each(firsts[:1], "wait_recv")
            each(firsts[:1], "wait_send")
            for d in range(3):
                edge_keep[d] = table(edge[6 + d], KEEP)
                edge_take[d] = table(edge[6 + d], TAKE)

        h_edge(slot)

        @pl.loop(0, 3)
        def _(g):
            for i in range(5):
                a = g * 5 + i
                h_plane(a, slot, E[X, a + 2], E[Z, a + 2])

        @pl.loop(0, 2)
        def _(g):
            for i in range(7):
                a = g * 7 + 1 + i
                e_plane(a)
                pack(a)

        each(copies[:4], "wait_recv")
        each(copies[:4], "wait_send")

        @pl.when(t == 0)
        def _():
            each(firsts[1:], "wait_recv")
            each(firsts[1:], "wait_send")
            for d in range(3):
                KP[d, 0] = table(G[d, 0], KEEP)
                TK[d, 0] = table(G[d, 0], TAKE)

        h_below(slot)
        h_plane(ny - 1, slot, y_high_in[slot, 0], y_high_in[slot, 1])
        h_edge_end(slot)
        e_plane(0)
        e_plane(ny - 1)
        pack_corners()

        @pl.when(t < steps - 1)
        def _():
            each(face_copies(1 - slot)[:4], "start")

        pack(0)
        pack(ny - 1)

        @pl.when(t < steps - 1)
        def _():
            each(face_copies(1 - slot)[4:], "start")

    stores = [
        pltpu.make_async_copy(field.at[SPOT[c], inner, x], out.at[c, x], store_sem.at[i, c, x])
        for i, (field, out) in enumerate(((E, eo_hbm), (H, ho_hbm)))
        for c in range(3)
        for x in range(nx)
    ]
    for copy in stores:
        copy.start()
    drive(steps - 1)
    rows, ports = half.shape
    members = (
        lax.broadcasted_iota(jnp.int32, (ports, slots), 0) == port_ref[...]
    ).astype(jnp.float32).astype(BF)
    high, low = halves(rec[...])
    total = dot_nt(high, members) + dot_nt(low, members)
    part[0] = total[0:rows]
    part[1] = total[rows : 2 * rows]

    def swap(number, source, target_ref):
        return pltpu.make_async_remote_copy(
            src_ref=source,
            dst_ref=target_ref,
            send_sem=pair_send.at[number],
            recv_sem=pair_recv.at[number],
            device_id=partner,
            device_id_type=MESH,
        )

    def send(axis, shift):
        return pltpu.make_async_remote_copy(
            src_ref=ring.at[axis, places[axis]],
            dst_ref=ring.at[axis, places[axis]],
            send_sem=ring_send.at[axis, shift],
            recv_sem=ring_recv.at[axis, shift],
            device_id=fellow(axis, shift),
            device_id_type=MESH,
        )

    def arrival(axis, shift):
        slot = (places[axis] + 4 - shift) % 4
        return pltpu.make_async_remote_copy(
            src_ref=ring.at[axis, slot],
            dst_ref=ring.at[axis, slot],
            send_sem=ring_send.at[axis, shift],
            recv_sem=ring_recv.at[axis, shift],
            device_id=fellow(axis, shift),
            device_id_type=MESH,
        )

    trade = swap(0, part.at[1 - core], half)
    trade.start()
    trade.wait()
    value = part[core] + half[...]
    for axis in range(3):
        ring[axis, places[axis]] = value
        for shift in range(1, 4):
            send(axis, shift).start()
        for shift in range(1, 4):
            arrival(axis, shift).wait_recv()
        value = (ring[axis, 0] + ring[axis, 1]) + (ring[axis, 2] + ring[axis, 3])
    whole[core] = value
    trade = swap(1, whole.at[core], whole.at[core])
    trade.start()
    for axis in range(3):
        for shift in range(1, 4):
            send(axis, shift).wait_send()
    trade.wait()
    pw_ref[0:rows] = whole[0]
    pw_ref[rows : 2 * rows] = whole[1]
    for copy in stores:
        copy.wait()


def local(
    electric, magnetic, aux_electric, aux_magnetic, grades, permittivity,
    dipole_cell, dipole_port, live_count, injection, waveform,
):
    shape = electric.shape[1:]
    nx, ny, nz = shape
    slots = dipole_cell.shape[1]
    ports, steps = waveform.shape
    f32 = jnp.float32
    anywhere = pl.BlockSpec(memory_space=pl.ANY)
    hbm = pl.BlockSpec(memory_space=pltpu.HBM)
    vmem = pl.BlockSpec(memory_space=pltpu.VMEM)
    half = (steps // 2, ports)
    return pl.pallas_call(
        functools.partial(kernel, shape, steps),
        out_shape=(
            jax.ShapeDtypeStruct(electric.shape, f32),
            jax.ShapeDtypeStruct(magnetic.shape, f32),
            jax.ShapeDtypeStruct((steps, ports), f32),
        ),
        in_specs=[pl.BlockSpec(memory_space=pltpu.SMEM)] + [hbm] * 10,
        out_specs=(anywhere, anywhere, vmem),
        scratch_shapes=[
            pltpu.VMEM((3, ny + 1, nx, nz), f32),
            pltpu.VMEM((3, ny + 1, nx, nz), f32),
            pltpu.VMEM((6, ny + 1, nx, nz), f32),
            pltpu.VMEM((6, ny, nx, nz), f32),
            pltpu.VMEM((3, ny + 1, nx, nz), jnp.int32),
            pltpu.VMEM((3, ny + 1, nx, nz), f32),
            pltpu.VMEM((3, ny + 1, nx, nz), f32),
            pltpu.VMEM((ny, nx, nz), f32),
            pltpu.VMEM((ny, nx, nz), f32),
            pltpu.VMEM((nx * ny, slots), f32),
            pltpu.VMEM((nz, slots), BF),
            pltpu.VMEM((steps, slots), f32),
            pltpu.VMEM((steps, slots), f32),
            pltpu.VMEM((nx * ny, nz), f32),
            pltpu.VMEM((2, 3, nx, nz), f32),
            pltpu.VMEM((2, 2, nx, nz), f32),
            pltpu.VMEM((2, 3, ny, nz), f32),
            pltpu.VMEM((2, 2, ny, nz), f32),
            pltpu.VMEM((2, 1, nz), f32),
            pltpu.VMEM((2, 1, nz), f32),
            pltpu.VMEM((2, ny, nz), f32),
            pltpu.VMEM((3, ny, nz), f32),
            pltpu.VMEM((1, nz), f32),
            pltpu.VMEM((1, nz), f32),
            pltpu.VMEM((9, ny, nz), f32),
            pltpu.VMEM((9, ny, nz), f32),
            pltpu.VMEM((3, ny, nz), f32),
            pltpu.VMEM((3, ny, nz), f32),
            pltpu.VMEM((3, slots), jnp.int32),
            pltpu.VMEM((1, slots), jnp.int32),
            pltpu.VMEM((slots, ports), BF),
            pltpu.VMEM((steps, ports), BF),
            pltpu.VMEM((2,) + half, f32),
            pltpu.VMEM(half, f32),
            pltpu.VMEM((3, 4) + half, f32),
            pltpu.VMEM((2,) + half, f32),
            pltpu.SemaphoreType.DMA((4,)),
            pltpu.SemaphoreType.DMA((10, ny)),
            pltpu.SemaphoreType.DMA((2, 3, nx)),
            pltpu.SemaphoreType.DMA((6,)),
            pltpu.SemaphoreType.DMA((6, 2)),
            pltpu.SemaphoreType.DMA((5,)),
            pltpu.SemaphoreType.DMA((5,)),
            pltpu.SemaphoreType.DMA((2,)),
            pltpu.SemaphoreType.DMA((2,)),
            pltpu.SemaphoreType.DMA((3, 4)),
            pltpu.SemaphoreType.DMA((3, 4)),
        ],
        compiler_params=pltpu.CompilerParams(
            collective_id=0, has_side_effects=True, vmem_limit_bytes=67_043_328
        ),
    )(
        live_count, electric, magnetic, aux_electric, aux_magnetic, grades, permittivity,
        dipole_cell, dipole_port.reshape(1, slots), injection, waveform.T,
    )


def solution(mesh):
    block = P(None, "gx", "gy", None)
    each = ("gx", "gy")
    return jax.shard_map(
        local,
        mesh=mesh,
        in_specs=(
            block, block, block, block, block, P("gx", "gy", None),
            P(None, each), P(each), P(each), P(each, None), P(),
        ),
        out_specs=(block, block, P()),
        check_vma=False,
    )
```
